32 devices in a mesh: dp: 1 (over z), tp: 32 (over x, y, core).
Axes of the slice: x: 4, y: 4, z: 1, core: 2. Of those that a mesh axis runs over, the one named last changes fastest.
The devices are a block of a 4x4x8 slice.
Arguments:
- x: bfloat16 [2048, 8192], P('dp')
- w_gate: bfloat16 [8192, 49152], P(None, 'tp')
- w_up: bfloat16 [8192, 49152], P(None, 'tp')
- w_down: bfloat16 [49152, 8192], P('tp')
Outputs:
- output: bfloat16 [2048, 8192], P('dp')
All inputs are finite; a program needn't handle non-finite values.
Results may differ from the reference program's by a relative error of at most 0.016.
Values are sent between devices in bfloat16 or wider.
A program may use at most 768 MiB of HBM per device.

```python
import jax
import jax.numpy as jnp

ROWS = 2048
D = 8192
FF = 49152


def setup_inputs(seed: int = 0, part: int = 0) -> dict:
    kx, kg, ku, kd = jax.random.split(jax.random.key(seed), 4)
    drawn = {
        "x": jax.random.normal(jax.random.fold_in(kx, part), (ROWS, D), jnp.float32),
        "w_gate": jax.random.normal(kg, (D, FF), jnp.float32) * D**-0.5,
        "w_up": jax.random.normal(ku, (D, FF), jnp.float32) * D**-0.5,
        "w_down": jax.random.normal(kd, (FF, D), jnp.float32) * FF**-0.5,
    }
    return {k: v.astype(jnp.bfloat16) for k, v in drawn.items()}


def reference(x, w_gate, w_up, w_down):
    gate = jnp.dot(x, w_gate, preferred_element_type=jnp.float32)
    up = jnp.dot(x, w_up, preferred_element_type=jnp.float32)
    hidden = (jax.nn.silu(gate) * up).astype(jnp.bfloat16)
    return jnp.dot(hidden, w_down, preferred_element_type=jnp.float32).astype(jnp.bfloat16)
```

```python
import functools
import math

import jax
import jax.numpy as jnp
from jax import lax
from jax.experimental import pallas as pl
from jax.experimental.pallas import tpu as pltpu
from jax.sharding import PartitionSpec as P

AXIS = "tp"
CORES = 2
RING = 4
STREAMS = 2
CHUNK = 512
FF_TILE = 256
UNITS = 4
TILES = 2
SLOTS = 4
FIRST = 15
OFFSETS = (0, 3, 5, 7, 9, 11, 13, 16, 18)
VMEM_LIMIT = 67_043_328


def _kernel(
    cfg, x_hbm, wg_hbm, wu_hbm, wd_hbm, y_hbm,
    x_v, h_v, wg_v, wu_v, wd_v, own, psend, precv, s1, r1, s2, r2, f1, fin,
    x_sem, wg_sem, wu_sem, wd_sem, pair_ss, pair_rs, s1_ss, s1_rs, s2_ss, s2_rs,
    g2_ss, g2_rs, g1_ss, g1_rs, loc_sem, share_ss, share_rs, credit,
):
    side, rows, chunk, ff_tile, unit = cfg
    n_chunks = rows // chunk
    n_units = n_chunks * UNITS
    n_ff = h_v.shape[1] // ff_tile
    gu_ticks = 2 * n_ff
    down_ticks = UNITS * TILES
    per_chunk = gu_ticks + down_ticks
    pace = per_chunk // UNITS
    tile = unit // TILES
    half_rows = chunk // CORES
    srows = half_rows // STREAMS
    brows = srows // RING
    bcols = unit // RING
    h1 = unit // 2
    h2 = bcols // 2
    xpiece = chunk // down_ticks

    me = lax.axis_index(AXIS)
    core = lax.rem(me, CORES)
    chip = lax.div(me, CORES)
    cx, cy = lax.div(chip, side), lax.rem(chip, side)

    def at(px, py):
        return (px * side + py) * CORES + core

    nxt = lambda v: lax.rem(v + 1, side)
    prv = lambda v: lax.rem(v + side - 1, side)
    xp, xm, yp, ym = at(nxt(cx), cy), at(prv(cx), cy), at(cx, nxt(cy)), at(cx, prv(cy))
    partner = chip * CORES + (1 - core)
    pos1, pos2 = (cx, cy), (cy, cx)
    ring1, ring2 = ((xp, xm), (yp, ym)), ((yp, ym), (xp, xm))

    bar = pltpu.get_barrier_semaphore()
    for d in (xp, xm, yp, ym, partner):
        pl.semaphore_signal(bar, inc=1, device_id={AXIS: d}, device_id_type=pl.DeviceIdType.MESH)
    pl.semaphore_wait(bar, 5)

    def remote(src, dst, ss, rs, dev):
        return pltpu.make_async_remote_copy(
            src_ref=src, dst_ref=dst, send_sem=ss, recv_sem=rs,
            device_id={AXIS: dev}, device_id_type=pl.DeviceIdType.MESH,
        )

    def w_copies(g):
        slot = lax.rem(g, 2)
        cols = pl.ds(pl.multiple_of(lax.rem(g, n_ff) * ff_tile, ff_tile), ff_tile)
        return (
            pltpu.make_async_copy(wg_hbm.at[:, cols], wg_v.at[slot], wg_sem.at[slot]),
            pltpu.make_async_copy(wu_hbm.at[:, cols], wu_v.at[slot], wu_sem.at[slot]),
        )

    def wd_copy(g):
        slot = lax.rem(g, 2)
        cols = pl.ds(pl.multiple_of(lax.rem(g, down_ticks) * tile, tile), tile)
        return pltpu.make_async_copy(wd_hbm.at[:, cols], wd_v.at[slot], wd_sem.at[slot])

    def x_copy(c, i):
        src = pl.ds(pl.multiple_of(c * chunk + i * xpiece, xpiece), xpiece)
        dst = pl.ds(pl.multiple_of(i * xpiece, xpiece), xpiece)
        return pltpu.make_async_copy(x_hbm.at[src], x_v.at[dst], x_sem.at[i])

    def pair_copy(u):
        ps, s = lax.rem(u, 2), lax.rem(u, SLOTS)
        return remote(psend.at[ps], precv.at[s], pair_ss.at[ps], pair_rs.at[s], partner)

    def rs_copy(ring, u, st, k):
        s = lax.rem(u, SLOTS)
        if ring == 1:
            sb, rb, ss, rs, nb = s1, r1, s1_ss, s1_rs, ring1
        else:
            sb, rb, ss, rs, nb = s2, r2, s2_ss, s2_rs, ring2
        return remote(sb.at[s, st, k], rb.at[s, st, k], ss.at[s, st, k], rs.at[s, st, k], nb[st][k % 2])

    def y_rows(u, st, q):
        base = lax.div(u, UNITS) * chunk + core * half_rows + st * srows + q * brows
        return pl.ds(pl.multiple_of(base, brows), brows)

    def y_cols(u, off, width):
        return pl.ds(pl.multiple_of(lax.rem(u, UNITS) * unit + off, width), width)

    def ag2_copy(u, st, k):
        s = lax.rem(u, SLOTS)
        p1, p2 = pos1[st], pos2[st]
        if k < 2:
            dst = y_hbm.at[y_rows(u, st, p1), y_cols(u, p2 * bcols, bcols)]
            src = fin.at[s, st]
        else:
            off = prv(p2) * bcols if k == 2 else nxt(p2) * bcols + h2
            src = dst = y_hbm.at[y_rows(u, st, p1), y_cols(u, off, h2)]
        return remote(src, dst, g2_ss.at[s, st, k], g2_rs.at[s, st, k], ring2[st][k % 2])

    def loc_copy(u, st):
        s = lax.rem(u, SLOTS)
        dst = y_hbm.at[y_rows(u, st, pos1[st]), y_cols(u, pos2[st] * bcols, bcols)]
        return pltpu.make_async_copy(fin.at[s, st], dst, loc_sem.at[s, st])

    def ag1_copy(u, st, k):
        s = lax.rem(u, SLOTS)
        p1 = pos1[st]
        if k < 2:
            part = y_hbm.at[y_rows(u, st, p1), y_cols(u, 0, unit)]
        elif k == 2:
            part = y_hbm.at[y_rows(u, st, prv(p1)), y_cols(u, 0, h1)]
        else:
            part = y_hbm.at[y_rows(u, st, nxt(p1)), y_cols(u, h1, h1)]
        return remote(part, part, g1_ss.at[s, st, k], g1_rs.at[s, st, k], ring1[st][k % 2])

    def share_copy(u):
        base = lax.div(u, UNITS) * chunk + core * half_rows
        part = y_hbm.at[pl.ds(pl.multiple_of(base, half_rows), half_rows), y_cols(u, 0, unit)]
        return remote(part, part, share_ss.at[u], share_rs.at[u], partner)

    f32 = lambda v: v.astype(jnp.float32)
    b16 = lambda v: v.astype(jnp.bfloat16)
    A1, B1 = pl.ds(0, h1), pl.ds(h1, h1)

    def rows_of(st, q):
        return pl.ds(pl.multiple_of(st * srows + q * brows, brows), brows)

    def stage_pair(u):
        s = lax.rem(u, SLOTS)
        pair_copy(u).wait_recv()
        for st in range(STREAMS):
            p = pos1[st]
            for d, cols, k in (
                (2, A1, 0), (2, B1, 1), (1, B1, 2), (3, A1, 3),
                (1, A1, None), (3, B1, None), (0, A1, None), (0, B1, None),
            ):
                r = rows_of(st, lax.rem(p + d, side))
                v = own[s, r, cols] + f32(precv[s, r, cols])
                if k is None:
                    own[s, r, cols] = v
                else:
                    s1[s, st, k] = b16(v)
        for k in range(4):
            for st in range(STREAMS):
                rs_copy(1, u, st, k).start()

        @pl.when(u + SLOTS < n_units)
        def _():
            pl.semaphore_signal(credit, inc=1, device_id={AXIS: partner}, device_id_type=pl.DeviceIdType.MESH)

    def stage_rs1_fwd(u):
        s = lax.rem(u, SLOTS)
        for st in range(STREAMS):
            p = pos1[st]
            rs_copy(1, u, st, 0).wait_recv()
            s1[s, st, 4] = b16(own[s, rows_of(st, nxt(p)), A1] + f32(r1[s, st, 0]))
            rs_copy(1, u, st, 1).wait_recv()
            s1[s, st, 5] = b16(own[s, rows_of(st, prv(p)), B1] + f32(r1[s, st, 1]))
        for k in (4, 5):
            for st in range(STREAMS):
                rs_copy(1, u, st, k).start()

    def stage_rs1_end(u):
        s = lax.rem(u, SLOTS)
        fs = lax.rem(u, 2)
        for st in range(STREAMS):
            r = rows_of(st, pos1[st])
            for k in (3, 4, 2, 5):
                rs_copy(1, u, st, k).wait_recv()
            f1[fs, st, :, A1] = own[s, r, A1] + f32(r1[s, st, 3]) + f32(r1[s, st, 4])
            f1[fs, st, :, B1] = own[s, r, B1] + f32(r1[s, st, 2]) + f32(r1[s, st, 5])
            for d, off, k in ((2, 0, 0), (2, h2, 1), (1, h2, 2), (3, 0, 3)):
                q = lax.rem(pos2[st] + d, side)
                s2[s, st, k] = b16(f1[fs, st, :, pl.ds(pl.multiple_of(q * bcols + off, h2), h2)])
        for k in range(4):
            for st in range(STREAMS):
                rs_copy(2, u, st, k).start()

    def f1_half(u, st, q, off):
        return f1[lax.rem(u, 2), st, :, pl.ds(pl.multiple_of(q * bcols + off, h2), h2)]

    def stage_rs2_fwd(u):
        s = lax.rem(u, SLOTS)
        for st in range(STREAMS):
            p = pos2[st]
            rs_copy(2, u, st, 0).wait_recv()
            s2[s, st, 4] = b16(f1_half(u, st, nxt(p), 0) + f32(r2[s, st, 0]))
            rs_copy(2, u, st, 1).wait_recv()
            s2[s, st, 5] = b16(f1_half(u, st, prv(p), h2) + f32(r2[s, st, 1]))
        for k in (4, 5):
            for st in range(STREAMS):
                rs_copy(2, u, st, k).start()

    def stage_rs2_end(u):
        s = lax.rem(u, SLOTS)
        for st in range(STREAMS):
            p = pos2[st]
            for k in (3, 4, 2, 5):
                rs_copy(2, u, st, k).wait_recv()
            a = f1_half(u, st, p, 0) + f32(r2[s, st, 3]) + f32(r2[s, st, 4])
            b = f1_half(u, st, p, h2) + f32(r2[s, st, 2]) + f32(r2[s, st, 5])
            fin[s, st, :, pl.ds(0, h2)] = b16(a)
            fin[s, st, :, pl.ds(h2, h2)] = b16(b)
        for st in range(STREAMS):
            for k in range(2):
                ag2_copy(u, st, k).start()
            loc_copy(u, st).start()

    def stage_ag2_fwd(u):
        for st in range(STREAMS):
            for k in range(2):
                ag2_copy(u, st, k).wait_recv()
                ag2_copy(u, st, k + 2).start()

    def stage_ag1(u):
        for st in range(STREAMS):
            loc_copy(u, st).wait()
            for k in (2, 3):
                ag2_copy(u, st, k).wait_recv()
            for k in range(2):
                ag1_copy(u, st, k).start()

    def stage_ag1_fwd(u):
        for st in range(STREAMS):
            for k in range(2):
                ag1_copy(u, st, k).wait_recv()
                ag1_copy(u, st, k + 2).start()

    def stage_share(u):
        for st in range(STREAMS):
            for k in (2, 3):
                ag1_copy(u, st, k).wait_recv()
        share_copy(u).start()
        for st in range(STREAMS):
            for k in range(6):
                rs_copy(1, u, st, k).wait_send()
                rs_copy(2, u, st, k).wait_send()
            for k in range(4):
                ag2_copy(u, st, k).wait_send()
                ag1_copy(u, st, k).wait_send()

    stages = (
        stage_pair, stage_rs1_fwd, stage_rs1_end, stage_rs2_fwd, stage_rs2_end,
        stage_ag2_fwd, stage_ag1, stage_ag1_fwd, stage_share,
    )

    def gate_up(c, tc):
        f, mh = lax.div(tc, 2), lax.rem(tc, 2)
        g = c * n_ff + f
        slot = lax.rem(g, 2)

        @pl.when(mh == 0)
        def _():
            for cp in w_copies(g):
                cp.wait()

            @pl.when(g + 1 < n_chunks * n_ff)
            def _():
                for cp in w_copies(g + 1):
                    cp.start()

        @pl.when(tc < 2)
        def _():
            for i in range(down_ticks // 2):
                x_copy(c, mh * (down_ticks // 2) + i).wait()

        m = pl.ds(pl.multiple_of(mh * half_rows, half_rows), half_rows)
        gate = jnp.dot(x_v[m, :], wg_v[slot], preferred_element_type=jnp.float32)
        up = jnp.dot(x_v[m, :], wu_v[slot], preferred_element_type=jnp.float32)
        cols = pl.ds(pl.multiple_of(f * ff_tile, ff_tile), ff_tile)
        h_v[m, cols] = b16(jax.nn.silu(gate) * up)

    def down(c, n):
        g = c * down_ticks + n
        j, i = lax.div(n, TILES), lax.rem(n, TILES)
        u = c * UNITS + j
        s, ps = lax.rem(u, SLOTS), lax.rem(u, 2)
        slot = lax.rem(g, 2)
        wd_copy(g).wait()

        @pl.when(g + 1 < n_chunks * down_ticks)
        def _():
            wd_copy(g + 1).start()

        @pl.when(c + 1 < n_chunks)
        def _():
            x_copy(c + 1, n).start()

        @pl.when((i == 0) & (u >= 2))
        def _():
            pair_copy(u - 2).wait_send()

        cols = pl.ds(pl.multiple_of(i * tile, tile), tile)
        theirs = pl.ds(pl.multiple_of((1 - core) * half_rows, half_rows), half_rows)
        mine = pl.ds(pl.multiple_of(core * half_rows, half_rows), half_rows)
        psend[ps, :, cols] = b16(jnp.dot(h_v[theirs, :], wd_v[slot], preferred_element_type=jnp.float32))
        own[s, :, cols] = jnp.dot(h_v[mine, :], wd_v[slot], preferred_element_type=jnp.float32)

        @pl.when(i == TILES - 1)
        def _():
            @pl.when(u >= SLOTS)
            def _():
                pl.semaphore_wait(credit, 1)

            pair_copy(u).start()

    for i in range(down_ticks // 2):
        x_copy(0, i).start()
    for cp in w_copies(0):
        cp.start()
    for i in range(down_ticks // 2, down_ticks):
        x_copy(0, i).start()
    wd_copy(0).start()

    total = (n_units - 1) * pace + FIRST + OFFSETS[-1] + 1

    def tick(t, carry):
        c, tc = lax.div(t, per_chunk), lax.rem(t, per_chunk)

        @pl.when((c < n_chunks) & (tc < gu_ticks))
        def _():
            gate_up(c, tc)

        @pl.when((c < n_chunks) & (tc >= gu_ticks))
        def _():
            down(c, tc - gu_ticks)

        for off, fn in reversed(tuple(zip(OFFSETS, stages))):
            e = t - FIRST - off
            u = lax.div(e, pace)

            @pl.when((e >= 0) & (lax.rem(e, pace) == 0) & (u < n_units))
            def _(u=u, fn=fn):
                fn(u)

        return carry

    lax.fori_loop(0, total, tick, 0)

    for u in (n_units - 2, n_units - 1):
        pair_copy(u).wait_send()

    def finish(u, carry):
        share_copy(u).wait()
        return carry

    lax.fori_loop(0, n_units, finish, 0)


def _mlp(mesh, chunk, ff_tile, x, w_gate, w_up, w_down):
    rows, d = x.shape
    ff = w_gate.shape[1]
    side = math.isqrt(mesh.shape[AXIS] // CORES)
    unit = d // UNITS
    tile = unit // TILES
    half_rows = chunk // CORES
    brows = half_rows // STREAMS // RING
    bcols = unit // RING
    n_units = rows // chunk * UNITS
    assert side == RING and side * side * CORES == mesh.shape[AXIS]
    assert 2 * (ff // ff_tile) + UNITS * TILES == UNITS * 5
    bf, dma = jnp.bfloat16, pltpu.SemaphoreType.DMA
    any_spec = pl.BlockSpec(memory_space=pl.ANY)
    return pl.pallas_call(
        functools.partial(_kernel, (side, rows, chunk, ff_tile, unit)),
        name="mlp_sum",
        out_shape=jax.ShapeDtypeStruct((rows, d), bf),
        in_specs=[any_spec] * 4,
        out_specs=any_spec,
        scratch_shapes=[
            pltpu.VMEM((chunk, d), bf),
            pltpu.VMEM((chunk, ff), bf),
            pltpu.VMEM((2, d, ff_tile), bf),
            pltpu.VMEM((2, d, ff_tile), bf),
            pltpu.VMEM((2, ff, tile), bf),
            pltpu.VMEM((SLOTS, half_rows, unit), jnp.float32),
            pltpu.VMEM((2, half_rows, unit), bf),
            pltpu.VMEM((SLOTS, half_rows, unit), bf),
            pltpu.VMEM((SLOTS, STREAMS, 6, brows, unit // 2), bf),
            pltpu.VMEM((SLOTS, STREAMS, 6, brows, unit // 2), bf),
            pltpu.VMEM((SLOTS, STREAMS, 6, brows, bcols // 2), bf),
            pltpu.VMEM((SLOTS, STREAMS, 6, brows, bcols // 2), bf),
            pltpu.VMEM((2, STREAMS, brows, unit), jnp.float32),
            pltpu.VMEM((SLOTS, STREAMS, brows, bcols), bf),
            dma((UNITS * TILES,)), dma((2,)), dma((2,)), dma((2,)),
            dma((2,)), dma((SLOTS,)),
            dma((SLOTS, STREAMS, 6)), dma((SLOTS, STREAMS, 6)),
            dma((SLOTS, STREAMS, 6)), dma((SLOTS, STREAMS, 6)),
            dma((SLOTS, STREAMS, 4)), dma((SLOTS, STREAMS, 4)),
            dma((SLOTS, STREAMS, 4)), dma((SLOTS, STREAMS, 4)),
            dma((SLOTS, STREAMS)), dma((n_units,)), dma((n_units,)),
            pltpu.SemaphoreType.REGULAR,
        ],
        compiler_params=pltpu.CompilerParams(
            collective_id=0, has_side_effects=True, vmem_limit_bytes=VMEM_LIMIT
        ),
        cost_estimate=pl.CostEstimate(
            flops=6 * rows * d * ff, bytes_accessed=3 * d * ff * 2 * (rows // chunk), transcendentals=rows * ff
        ),
    )(x, w_gate, w_up, w_down)


def solution(mesh):
    return jax.shard_map(
        functools.partial(_mlp, mesh, CHUNK, FF_TILE),
        mesh=mesh,
        in_specs=(P("dp", None), P(None, AXIS), P(None, AXIS), P(AXIS, None)),
        out_specs=P("dp", None),
        check_vma=False,
    )
```

```python
import functools
import math

import jax
import jax.numpy as jnp
from jax import lax
from jax.experimental import pallas as pl
from jax.experimental.pallas import tpu as pltpu
from jax.sharding import PartitionSpec as P

AXIS = "tp"
CORES = 2
RING = 4
STREAMS = 2
CHUNK = 512
FF_TILE = 256
UNITS = 8
TILES = 1
SLOTS = 8
GATHERS = 16
FIRST = 14
STEP = 1
OFFSETS = (0, 2, 4, 6, 8, 10, 12, 15, 17)
VMEM_LIMIT = 67_043_328


def _kernel(
    cfg, x_hbm, wg_hbm, wu_hbm, wd_hbm, y_hbm,
    x_v, h_v, wg_v, wu_v, wd_v, own, psend, precv, s1, r1, s2, r2, f1, fin,
    x_sem, wg_sem, wu_sem, wd_sem, pair_ss, pair_rs, s1_ss, s1_rs, s2_ss, s2_rs,
    g2_ss, g2_rs, g1_ss, g1_rs, loc_sem, share_ss, share_rs, credit,
):
    side, rows, chunk, ff_tile, unit = cfg
    n_chunks = rows // chunk
    n_units = n_chunks * UNITS
    n_ff = h_v.shape[1] // ff_tile
    gu_ticks = 2 * n_ff
    down_ticks = UNITS * TILES
    per_chunk = gu_ticks + down_ticks
    tile = unit // TILES
    half_rows = chunk // CORES
    srows = half_rows // STREAMS
    brows = srows // RING
    bcols = unit // RING
    h1 = unit // 2
    h2 = bcols // 2
    xpiece = chunk // down_ticks

    me = lax.axis_index(AXIS)
    core = lax.rem(me, CORES)
    chip = lax.div(me, CORES)
    cx, cy = lax.div(chip, side), lax.rem(chip, side)

    def at(px, py):
        return (px * side + py) * CORES + core

    nxt = lambda v: lax.rem(v + 1, side)
    prv = lambda v: lax.rem(v + side - 1, side)
    xp, xm, yp, ym = at(nxt(cx), cy), at(prv(cx), cy), at(cx, nxt(cy)), at(cx, prv(cy))
    partner = chip * CORES + (1 - core)
    pos1, pos2 = (cx, cy), (cy, cx)
    ring1, ring2 = ((xp, xm), (yp, ym)), ((yp, ym), (xp, xm))

    bar = pltpu.get_barrier_semaphore()
    for d in (xp, xm, yp, ym, partner):
        pl.semaphore_signal(bar, inc=1, device_id={AXIS: d}, device_id_type=pl.DeviceIdType.MESH)
    pl.semaphore_wait(bar, 5)

    def remote(src, dst, ss, rs, dev):
        return pltpu.make_async_remote_copy(
            src_ref=src, dst_ref=dst, send_sem=ss, recv_sem=rs,
            device_id={AXIS: dev}, device_id_type=pl.DeviceIdType.MESH,
        )

    def w_copies(g):
        slot = lax.rem(g, 2)
        cols = pl.ds(pl.multiple_of(lax.rem(g, n_ff) * ff_tile, ff_tile), ff_tile)
        return (
            pltpu.make_async_copy(wg_hbm.at[:, cols], wg_v.at[slot], wg_sem.at[slot]),
            pltpu.make_async_copy(wu_hbm.at[:, cols], wu_v.at[slot], wu_sem.at[slot]),
        )

    def wd_copy(g):
        slot = lax.rem(g, 2)
        cols = pl.ds(pl.multiple_of(lax.rem(g, down_ticks) * tile, tile), tile)
        return pltpu.make_async_copy(wd_hbm.at[:, cols], wd_v.at[slot], wd_sem.at[slot])

    def x_copy(c, i):
        src = pl.ds(pl.multiple_of(c * chunk + i * xpiece, xpiece), xpiece)
        dst = pl.ds(pl.multiple_of(i * xpiece, xpiece), xpiece)
        return pltpu.make_async_copy(x_hbm.at[src], x_v.at[dst], x_sem.at[i])

    def pair_copy(u):
        ps, s = lax.rem(u, 2), lax.rem(u, SLOTS)
        return remote(psend.at[ps], precv.at[s], pair_ss.at[ps], pair_rs.at[s], partner)

    def ring_refs(ring):
        return (s1, r1, s1_ss, s1_rs, ring1) if ring == 1 else (s2, r2, s2_ss, s2_rs, ring2)

    def rs_copy(ring, u, st, k):
        s = lax.rem(u, SLOTS)
        sb, rb, ss, rs, nb = ring_refs(ring)
        part = pl.ds(2 * k, 2) if k < 2 else k + 2
        return remote(sb.at[s, st, part], rb.at[s, st, part], ss.at[s], rs.at[s, k // 2], nb[st][k % 2])

    def landed(ref, sem):
        pltpu.make_async_copy(ref, ref, sem).wait()

    def rs_landed(ring, u, step):
        s = lax.rem(u, SLOTS)
        _, rb, _, rs, _ = ring_refs(ring)
        landed(rb.at[s, :, pl.ds(4 * step, 4 - 2 * step)], rs.at[s, step])

    def rs_sent(ring, u):
        s = lax.rem(u, SLOTS)
        sb, _, ss, _, _ = ring_refs(ring)
        landed(sb.at[s], ss.at[s])

    def y_rows(u, st, q):
        base = lax.div(u, UNITS) * chunk + core * half_rows + st * srows + q * brows
        return pl.ds(pl.multiple_of(base, brows), brows)

    def y_cols(u, off, width):
        return pl.ds(pl.multiple_of(lax.rem(u, UNITS) * unit + off, width), width)

    def ag2_copy(u, st, k):
        s = lax.rem(u, GATHERS)
        p1, p2 = pos1[st], pos2[st]
        if k < 2:
            dst = y_hbm.at[y_rows(u, st, p1), y_cols(u, p2 * bcols, bcols)]
            src = fin.at[s, st]
        else:
            off = prv(p2) * bcols if k == 2 else nxt(p2) * bcols + h2
            src = dst = y_hbm.at[y_rows(u, st, p1), y_cols(u, off, h2)]
        return remote(src, dst, g2_ss.at[s], g2_rs.at[s, k // 2], ring2[st][k % 2])

    def loc_copy(u, st):
        s = lax.rem(u, GATHERS)
        dst = y_hbm.at[y_rows(u, st, pos1[st]), y_cols(u, pos2[st] * bcols, bcols)]
        return pltpu.make_async_copy(fin.at[s, st], dst, loc_sem.at[s])

    def ag1_copy(u, st, k):
        s = lax.rem(u, GATHERS)
        p1 = pos1[st]
        if k < 2:
            part = y_hbm.at[y_rows(u, st, p1), y_cols(u, 0, unit)]
        elif k == 2:
            part = y_hbm.at[y_rows(u, st, prv(p1)), y_cols(u, 0, h1)]
        else:
            part = y_hbm.at[y_rows(u, st, nxt(p1)), y_cols(u, h1, h1)]
        return remote(part, part, g1_ss.at[s], g1_rs.at[s, k // 2], ring1[st][k % 2])

    def ag_landed(ring, u, step):
        s = lax.rem(u, GATHERS)
        rows_, cols_ = (brows, unit) if ring == 2 else (brows * RING, unit)
        part = y_hbm.at[pl.ds(0, rows_ // (1 + step)), pl.ds(0, cols_)]
        landed(part, (g1_rs if ring == 1 else g2_rs).at[s, step])

    def ag_sent(u):
        s = lax.rem(u, GATHERS)
        for sem, n in ((g2_ss, brows), (g1_ss, brows * RING)):
            landed(y_hbm.at[pl.ds(0, n + n // 2), pl.ds(0, unit)], sem.at[s])

    def share_copy(u):
        base = lax.div(u, UNITS) * chunk + core * half_rows
        part = y_hbm.at[pl.ds(pl.multiple_of(base, half_rows), half_rows), y_cols(u, 0, unit)]
        return remote(part, part, share_ss.at[u], share_rs.at[u], partner)

    f32 = lambda v: v.astype(jnp.float32)
    b16 = lambda v: v.astype(jnp.bfloat16)
    A1, B1 = pl.ds(0, h1), pl.ds(h1, h1)

    def rows_of(st, q):
        return pl.ds(pl.multiple_of(st * srows + q * brows, brows), brows)

    def chip_sum(s, st, q, cols):
        r = rows_of(st, q)
        return own[s, r, cols] + f32(precv[s, r, cols])

    def f1_half(u, st, q, off):
        return f1[lax.rem(u, SLOTS), st, :, pl.ds(pl.multiple_of(q * bcols + off, h2), h2)]

    def stage_pair(u):
        s = lax.rem(u, SLOTS)
        pair_copy(u).wait_recv()
        for st in range(STREAMS):
            p = pos1[st]
            for d, cols, k in ((2, A1, 0), (1, B1, 1), (2, B1, 2), (3, A1, 3)):
                s1[s, st, k] = b16(chip_sum(s, st, lax.rem(p + d, side), cols))
        for k in range(2):
            for st in range(STREAMS):
                rs_copy(1, u, st, k).start()

    def stage_rs1_fwd(u):
        s = lax.rem(u, SLOTS)
        rs_landed(1, u, 0)
        for st in range(STREAMS):
            p = pos1[st]
            s1[s, st, 4] = b16(chip_sum(s, st, nxt(p), A1) + f32(r1[s, st, 0]))
            s1[s, st, 5] = b16(chip_sum(s, st, prv(p), B1) + f32(r1[s, st, 2]))
        for k in (2, 3):
            for st in range(STREAMS):
                rs_copy(1, u, st, k).start()

    def stage_rs1_end(u):
        s = lax.rem(u, SLOTS)
        rs_landed(1, u, 1)
        for st in range(STREAMS):
            p = pos1[st]
            f1[s, st, :, A1] = chip_sum(s, st, p, A1) + f32(r1[s, st, 3]) + f32(r1[s, st, 4])
            f1[s, st, :, B1] = chip_sum(s, st, p, B1) + f32(r1[s, st, 1]) + f32(r1[s, st, 5])
            for d, off, k in ((2, 0, 0), (1, h2, 1), (2, h2, 2), (3, 0, 3)):
                s2[s, st, k] = b16(f1_half(u, st, lax.rem(pos2[st] + d, side), off))
        for k in range(2):
            for st in range(STREAMS):
                rs_copy(2, u, st, k).start()

        @pl.when(u + SLOTS < n_units)
        def _():
            pl.semaphore_signal(credit, inc=1, device_id={AXIS: partner}, device_id_type=pl.DeviceIdType.MESH)

    def stage_rs2_fwd(u):
        s = lax.rem(u, SLOTS)
        rs_landed(2, u, 0)
        for st in range(STREAMS):
            p = pos2[st]
            s2[s, st, 4] = b16(f1_half(u, st, nxt(p), 0) + f32(r2[s, st, 0]))
            s2[s, st, 5] = b16(f1_half(u, st, prv(p), h2) + f32(r2[s, st, 2]))
        for k in (2, 3):
            for st in range(STREAMS):
                rs_copy(2, u, st, k).start()

    def stage_rs2_end(u):
        s, gs = lax.rem(u, SLOTS), lax.rem(u, GATHERS)
        rs_landed(2, u, 1)
        for st in range(STREAMS):
            p = pos2[st]
            a = f1_half(u, st, p, 0) + f32(r2[s, st, 3]) + f32(r2[s, st, 4])
            b = f1_half(u, st, p, h2) + f32(r2[s, st, 1]) + f32(r2[s, st, 5])
            fin[gs, st, :, pl.ds(0, h2)] = b16(a)
            fin[gs, st, :, pl.ds(h2, h2)] = b16(b)
        for st in range(STREAMS):
            for k in range(2):
                ag2_copy(u, st, k).start()
            loc_copy(u, st).start()
        rs_sent(1, u)

    def stage_ag2_fwd(u):
        ag_landed(2, u, 0)
        for st in range(STREAMS):
            for k in (2, 3):
                ag2_copy(u, st, k).start()

    def stage_ag1(u):
        landed(fin.at[lax.rem(u, GATHERS)], loc_sem.at[lax.rem(u, GATHERS)])
        ag_landed(2, u, 1)
        for st in range(STREAMS):
            for k in range(2):
                ag1_copy(u, st, k).start()
        rs_sent(2, u)

    def stage_ag1_fwd(u):
        ag_landed(1, u, 0)
        for st in range(STREAMS):
            for k in (2, 3):
                ag1_copy(u, st, k).start()

    def stage_share(u):
        ag_landed(1, u, 1)
        share_copy(u).start()
        ag_sent(u)

    stages = (
        stage_pair, stage_rs1_fwd, stage_rs1_end, stage_rs2_fwd, stage_rs2_end,
        stage_ag2_fwd, stage_ag1, stage_ag1_fwd, stage_share,
    )

    def gate_up(c, tc):
        f, mh = lax.div(tc, 2), lax.rem(tc, 2)
        g = c * n_ff + f
        slot = lax.rem(g, 2)

        @pl.when(mh == 0)
        def _():
            for cp in w_copies(g):
                cp.wait()

            @pl.when(g + 1 < n_chunks * n_ff)
            def _():
                for cp in w_copies(g + 1):
                    cp.start()

        @pl.when(tc < 2)
        def _():
            for i in range(down_ticks // 2):
                x_copy(c, mh * (down_ticks // 2) + i).wait()

        m = pl.ds(pl.multiple_of(mh * half_rows, half_rows), half_rows)
        gate = jnp.dot(x_v[m, :], wg_v[slot], preferred_element_type=jnp.float32)
        up = jnp.dot(x_v[m, :], wu_v[slot], preferred_element_type=jnp.float32)
        cols = pl.ds(pl.multiple_of(f * ff_tile, ff_tile), ff_tile)
        h_v[m, cols] = b16(jax.nn.silu(gate) * up)

    def down(c, n):
        g = c * down_ticks + n
        j, i = lax.div(n, TILES), lax.rem(n, TILES)
        u = c * UNITS + j
        s, ps = lax.rem(u, SLOTS), lax.rem(u, 2)
        slot = lax.rem(g, 2)
        wd_copy(g).wait()

        @pl.when(g + 1 < n_chunks * down_ticks)
        def _():
            wd_copy(g + 1).start()

        @pl.when(c + 1 < n_chunks)
        def _():
            x_copy(c + 1, n).start()

        @pl.when((i == 0) & (u >= 2))
        def _():
            pair_copy(u - 2).wait_send()

        cols = pl.ds(pl.multiple_of(i * tile, tile), tile)
        theirs = pl.ds(pl.multiple_of((1 - core) * half_rows, half_rows), half_rows)
        mine = pl.ds(pl.multiple_of(core * half_rows, half_rows), half_rows)
        psend[ps, :, cols] = b16(jnp.dot(h_v[theirs, :], wd_v[slot], preferred_element_type=jnp.float32))
        own[s, :, cols] = jnp.dot(h_v[mine, :], wd_v[slot], preferred_element_type=jnp.float32)

        @pl.when(i == TILES - 1)
        def _():
            @pl.when(u >= SLOTS)
            def _():
                pl.semaphore_wait(credit, 1)

            pair_copy(u).start()

    for i in range(down_ticks // 2):
        x_copy(0, i).start()
    for cp in w_copies(0):
        cp.start()
    for i in range(down_ticks // 2, down_ticks):
        x_copy(0, i).start()
    wd_copy(0).start()

    total = (n_chunks - 1) * per_chunk + (UNITS - 1) * STEP + FIRST + OFFSETS[-1] + 1

    def tick(t, carry):
        c, tc = lax.div(t, per_chunk), lax.rem(t, per_chunk)

        @pl.when((c < n_chunks) & (tc < gu_ticks))
        def _():
            gate_up(c, tc)

        @pl.when((c < n_chunks) & (tc >= gu_ticks))
        def _():
            down(c, tc - gu_ticks)

        for off, fn in zip(OFFSETS, stages):
            e = t - FIRST - off
            j = lax.rem(e, per_chunk)
            u = lax.div(e, per_chunk) * UNITS + lax.div(j, STEP)

            @pl.when((e >= 0) & (lax.rem(j, STEP) == 0) & (j < UNITS * STEP) & (u < n_units))
            def _(u=u, fn=fn):
                fn(u)

        return carry

    lax.fori_loop(0, total, tick, 0)

    for u in (n_units - 2, n_units - 1):
        pair_copy(u).wait_send()

    def finish(u, carry):
        share_copy(u).wait()
        return carry

    lax.fori_loop(0, n_units, finish, 0)


def _mlp(mesh, chunk, ff_tile, x, w_gate, w_up, w_down):
    rows, d = x.shape
    ff = w_gate.shape[1]
    side = math.isqrt(mesh.shape[AXIS] // CORES)
    unit = d // UNITS
    tile = unit // TILES
    half_rows = chunk // CORES
    brows = half_rows // STREAMS // RING
    bcols = unit // RING
    n_units = rows // chunk * UNITS
    assert side == RING and side * side * CORES == mesh.shape[AXIS]
    assert 2 * (ff // ff_tile) + UNITS * TILES == 5 * UNITS * TILES // 2
    bf, dma = jnp.bfloat16, pltpu.SemaphoreType.DMA
    any_spec = pl.BlockSpec(memory_space=pl.ANY)
    return pl.pallas_call(
        functools.partial(_kernel, (side, rows, chunk, ff_tile, unit)),
        name="mlp_sum",
        out_shape=jax.ShapeDtypeStruct((rows, d), bf),
        in_specs=[any_spec] * 4,
        out_specs=any_spec,
        scratch_shapes=[
            pltpu.VMEM((chunk, d), bf),
            pltpu.VMEM((chunk, ff), bf),
            pltpu.VMEM((2, d, ff_tile), bf),
            pltpu.VMEM((2, d, ff_tile), bf),
            pltpu.VMEM((2, ff, tile), bf),
            pltpu.VMEM((SLOTS, half_rows, unit), jnp.float32),
            pltpu.VMEM((2, half_rows, unit), bf),
            pltpu.VMEM((SLOTS, half_rows, unit), bf),
            pltpu.VMEM((SLOTS, STREAMS, 6, brows, unit // 2), bf),
            pltpu.VMEM((SLOTS, STREAMS, 6, brows, unit // 2), bf),
            pltpu.VMEM((SLOTS, STREAMS, 6, brows, bcols // 2), bf),
            pltpu.VMEM((SLOTS, STREAMS, 6, brows, bcols // 2), bf),
            pltpu.VMEM((SLOTS, STREAMS, brows, unit), jnp.float32),
            pltpu.VMEM((GATHERS, STREAMS, brows, bcols), bf),
            dma((UNITS * TILES,)), dma((2,)), dma((2,)), dma((2,)),
            dma((2,)), dma((SLOTS,)),
            dma((SLOTS,)), dma((SLOTS, 2)), dma((SLOTS,)), dma((SLOTS, 2)),
            dma((GATHERS,)), dma((GATHERS, 2)), dma((GATHERS,)), dma((GATHERS, 2)),
            dma((GATHERS,)), dma((n_units,)), dma((n_units,)),
            pltpu.SemaphoreType.REGULAR,
        ],
        compiler_params=pltpu.CompilerParams(
            collective_id=0, has_side_effects=True, vmem_limit_bytes=VMEM_LIMIT
        ),
        cost_estimate=pl.CostEstimate(
            flops=6 * rows * d * ff, bytes_accessed=3 * d * ff * 2 * (rows // chunk), transcendentals=rows * ff
        ),
    )(x, w_gate, w_up, w_down)


def solution(mesh):
    return jax.shard_map(
        functools.partial(_mlp, mesh, CHUNK, FF_TILE),
        mesh=mesh,
        in_specs=(P("dp", None), P(None, AXIS), P(None, AXIS), P(AXIS, None)),
        out_specs=P("dp", None),
        check_vma=False,
    )
```
